256 devices in a mesh: site: 32 (over z, y), ka: 8 (over x, core).
Axes of the slice: x: 4, y: 4, z: 8, core: 2. Of those that a mesh axis runs over, the one named last changes fastest.
Arguments:
- positions: float32 [3, 512], P(None, 'site'), may hold values from 0 to 1
- site_class: int32 [512], P('site'), may hold values from 0 to 3
- class_charge: float32 [4], replicated, may hold values from -2 to 2
- miller: int32 [3, 1048576], P(None, 'ka'), may hold values from -80 to 80, as said below
Outputs:
- forces: float32 [3, 512], P(None, ('site', 'ka'))
- energy: float32 [], replicated
The draws below stay inside these ranges and needn't reach their ends.
Inputs may be any that keep to these rules, and one draw needn't show every extreme that they name: `miller`: the k-vectors are all distinct, and none has all three indices zero.
All inputs are finite; a program needn't handle non-finite values.
Results may differ from the reference program's by a relative error of at most 0.0003.
Values sent between devices are 32-bit elements; how exact they have to be, the bound alone decides.
A program may use at most 64 MiB of HBM per device.

```python
import math
import jax
import jax.numpy as jnp
from jax import lax

KBLOCK = 4096
MMAX = 80
NCLS = 4
NSITES = 512
KVECS = 1048576


def draw_miller(key, part):
    side = 2 * MMAX + 1
    cube = side * side * side
    centre = (cube - 1) // 2
    order = jax.random.permutation(jax.random.fold_in(key, 11), cube - 1).astype(jnp.int32)
    picked = order[:KVECS]
    picked = jnp.where(picked >= centre, picked + 1, picked)
    first = picked // (side * side) - MMAX
    second = picked // side % side - MMAX
    third = picked % side - MMAX
    return jnp.stack([first, second, third], axis=0).astype(jnp.int32)


def place_ends(values, rng, low, top_value):
    longest = values.shape.index(max(values.shape))
    spots = []
    for shift in (0, 1):
        where = [jax.random.randint(jax.random.fold_in(rng, axis), (), 0, length) for axis, length in enumerate(values.shape)]
        where[longest] = (where[longest] + shift) % values.shape[longest]
        spots.append(tuple(where))
    return values.at[spots[0]].set(low).at[spots[1]].set(top_value)


def level_of(rng, extent, cuts, smallest, top_value):
    loudness, own = 1.0, jax.random.fold_in(rng, 6)
    for axis_at, shards_of in cuts:
        steps = jnp.exp(jax.random.uniform(jax.random.fold_in(own, axis_at), (shards_of,), jnp.float32, smallest / len(cuts), top_value / len(cuts)))
        loudness = loudness * jnp.repeat(steps, extent[axis_at] // shards_of).reshape([-1 if axis == axis_at else 1 for axis in range(len(extent))])
    return loudness


def setup_inputs(seed: int = 0) -> dict:
    key_of = jax.random.split(jax.random.key(seed), 5)
    positions = jnp.clip(1.0 * jax.random.uniform(key_of[0], (3, NSITES), jnp.float32) ** level_of(key_of[0], (3, NSITES), ((1, 32),), -0.2, 0.2), 0.0, 1.0)
    site_class = place_ends(jax.random.randint(key_of[1], (NSITES,), 0, NCLS), jax.random.fold_in(key_of[1], 1), 0, NCLS - 1).astype(jnp.int32)
    class_charge = jnp.clip(jax.random.uniform(key_of[2], (NCLS,), jnp.float32, -2.0, 2.0), -2.0, 2.0)
    miller = draw_miller(jax.random.fold_in(key_of[4], 71), 0)
    return dict(positions=positions, site_class=site_class, class_charge=class_charge, miller=miller)


def charges_of(site_class, class_charge):
    onehot = (site_class[None, :] == jnp.arange(NCLS, dtype=jnp.int32)[:, None]).astype(jnp.float32)
    return jnp.dot(class_charge, onehot, precision=lax.Precision.HIGHEST)

def kernel_weights(mfloat):
    square = lax.optimization_barrier(jnp.sum(mfloat * mfloat, axis=0))
    limit = float(MMAX * MMAX)
    return limit * jnp.exp(-square / limit) / square

def phases(mblock, positions):
    angles = 2.0 * math.pi * (mblock[0][:, None] * positions[0][None, :] + mblock[1][:, None] * positions[1][None, :] + mblock[2][:, None] * positions[2][None, :])
    return (jnp.cos(angles), jnp.sin(angles))

def reference(positions, site_class, class_charge, miller):
    charge = charges_of(site_class, class_charge)
    mfloat = miller.astype(jnp.float32)
    weights = kernel_weights(mfloat)
    blocks = KVECS // KBLOCK
    mblocks = mfloat.reshape(3, blocks, KBLOCK).transpose(1, 0, 2)
    scale = 1.0 / math.sqrt(NSITES)

    def factor(mblock):
        cosine, sine = phases(mblock, positions)
        return (jnp.dot(cosine, charge, precision=lax.Precision.HIGHEST) * scale, jnp.dot(sine, charge, precision=lax.Precision.HIGHEST) * scale)
    creal, cimag = lax.map(factor, mblocks)
    wblocks = weights.reshape(blocks, KBLOCK)
    energy = jnp.sum(wblocks * (creal * creal + cimag * cimag)) / KVECS

    def accumulate(total, items):
        mblock, real_part, imag_part, wblock = items
        cosine, sine = phases(mblock, positions)
        grad_sine = mblock * (wblock * real_part)[None, :]
        grad_cosine = mblock * (wblock * imag_part)[None, :]
        total = total + jnp.dot(grad_sine, sine, precision=lax.Precision.HIGHEST) - jnp.dot(grad_cosine, cosine, precision=lax.Precision.HIGHEST)
        return (total, None)
    total, unused = lax.scan(accumulate, jnp.zeros((3, NSITES), jnp.float32), (mblocks, creal, cimag, wblocks))
    forces = 4.0 * math.pi / math.sqrt(NSITES * KVECS) * charge[None, :] * total
    return (forces, energy)
```

```python
import functools
import math

import jax
import jax.numpy as jnp
from jax import lax
from jax.experimental import pallas as pl
from jax.experimental.pallas import tpu as pltpu
from jax.sharding import Mesh
from jax.sharding import PartitionSpec as P

MMAX = 80
NCLS = 4
SITE = ("site_0", "site_1")
KA = ("ka_0", "ka_1")
SITE_KA = ("site_0", "site_1", "ka_0", "ka_1")
AXES = SITE_KA
MESH = pl.DeviceIdType.MESH
BLOCK = 256
LANES = 128
GROUP = 16
SINE = (4.442840086703501, -7.306690622039078, 3.589268246765133, -0.7724978545428361)


def offsets(far, near):
    steps = [(a, b) for a in range(far) for b in range(near)]
    return sorted(steps, key=lambda s: (min(s[0], far - s[0]) + min(s[1], near - s[1]), s))


def rounded(value):
    return value.astype(jnp.bfloat16).astype(jnp.float32)


def three_parts(value):
    high = rounded(value)
    middle = rounded(value - high)
    return high, middle, value - high - middle


def kernel(
    sizes,
    kvecs_all,
    positions,
    site_class,
    class_charge,
    miller,
    forces,
    energy,
    mints,
    xrows,
    columns,
    weight,
    table,
    angle,
    cosine,
    sine,
    creal,
    cimag,
    outbox,
    inbox,
    shared,
    mine_sem,
    site_send,
    site_recv,
    force_send,
    force_recv,
    last_send,
    last_recv,
):
    nz, ny, nx, nc = sizes
    kvecs = mints.shape[1]
    blocks = kvecs // BLOCK
    slots = offsets(nz, ny)
    mates = offsets(nx, nc)
    chunks = len(slots) // 8
    nsites = len(slots) * GROUP
    z, y, x, c = (lax.axis_index(axis) for axis in AXES)

    def at(dz, dy, dx, dc):
        return (lax.rem(z + dz, nz), lax.rem(y + dy, ny), lax.rem(x + dx, nx), lax.rem(c + dc, nc))

    start = pl.multiple_of((z * ny + y) * kvecs, LANES)
    fetch = pltpu.make_async_copy(miller.at[:, pl.ds(start, kvecs)], mints, mine_sem)
    fetch.start()
    barrier = pltpu.get_barrier_semaphore()
    for dz, dy in slots[1:]:
        pl.semaphore_signal(barrier, inc=1, device_id=at(dz, dy, 0, 0), device_id_type=MESH)
    for dx, dc in mates[1:]:
        pl.semaphore_signal(barrier, inc=1, device_id=at(0, 0, dx, dc), device_id_type=MESH)

    classes = site_class[...]
    charge = jnp.zeros(classes.shape, jnp.float32)
    for index in range(NCLS):
        charge = jnp.where(classes == index, class_charge[index], charge)
    place = positions[...]
    place = place - jnp.round(place)
    table[0] = jnp.concatenate(
        [place[0:1], place[1:2], place[2:3], charge, jnp.zeros((1, LANES - 4 * GROUP), jnp.float32)], axis=1
    )

    fetch.wait()
    limit = float(MMAX * MMAX)

    def prepare(block, carry):
        here = pl.ds(pl.multiple_of(block * BLOCK, BLOCK), BLOCK)
        m = mints[:, here].astype(jnp.float32)
        square = m[0:1] * m[0:1] + m[1:2] * m[1:2] + m[2:3] * m[2:3]
        w = limit * jnp.exp(-square / limit) / square
        rows = jnp.concatenate([m, m, m, *three_parts(w), jnp.zeros((4, BLOCK), jnp.float32)], axis=0)
        xrows[:, here] = rows.astype(jnp.bfloat16)
        columns[here, :] = rows.T.astype(jnp.bfloat16)
        return carry

    lax.fori_loop(0, blocks, prepare, 0)
    row = lax.broadcasted_iota(jnp.int32, (16, LANES), 0)
    picks = jnp.where((row >= 9) & (row < 12), 1.0, 0.0).astype(jnp.bfloat16)

    def spread(block, carry):
        here = pl.ds(pl.multiple_of(block * BLOCK, BLOCK), BLOCK)
        weight[here, :] = jnp.dot(columns[here, :], picks, preferred_element_type=jnp.float32)
        return carry

    lax.fori_loop(0, blocks, spread, 0)

    pl.semaphore_wait(barrier, len(slots) + len(mates) - 2)
    sends = [None]
    for slot, (dz, dy) in enumerate(slots):
        if slot:
            copy = pltpu.make_async_remote_copy(
                src_ref=table.at[0],
                dst_ref=table.at[slot],
                send_sem=site_send.at[slot],
                recv_sem=site_recv.at[slot],
                device_id=at(dz, dy, 0, 0),
                device_id_type=MESH,
            )
            copy.start()
            sends.append(copy)

    lane = lax.broadcasted_iota(jnp.int32, (8, LANES), 1)
    sublane = lax.broadcasted_iota(jnp.int32, (8, LANES), 0)
    group = lane // GROUP

    def unpack(chunk):
        got = table[pl.ds(8 * chunk, 8), 0, :]
        rolled = [got if r == 0 else pltpu.roll(got, GROUP * r, axis=1) for r in range(8)]
        out = []
        for d in range(4):
            value = jnp.zeros((8, LANES), jnp.float32)
            for s in range(8):
                value = jnp.where((sublane == s) & (group == s), rolled[(s - d) % 8], value)
            out.append(jnp.sum(value, axis=0, keepdims=True))
        coords = jnp.concatenate(out[:3], axis=0)
        parts = jnp.concatenate([*three_parts(coords), jnp.zeros((7, LANES), jnp.float32)], axis=0)
        return parts.astype(jnp.bfloat16), out[3]

    def angles(block, parts):
        here = pl.ds(pl.multiple_of(block * BLOCK, BLOCK), BLOCK)
        return jnp.dot(columns[here, :], parts, preferred_element_type=jnp.float32)

    def phase_one(chunk, parts, charges, first, last):
        half, lanes = chunk // 2, pl.ds((chunk % 2) * LANES, LANES)
        angle[0] = angles(0, parts)

        def step(block, total):
            following = angles(lax.rem(block + 1, blocks), parts)
            slot = lax.rem(block, 2)
            base = block * BLOCK
            for sub in range(BLOCK // 64):
                here = pl.ds(pl.multiple_of(base + sub * 64, 64), 64)
                turns = angle[slot, pl.ds(sub * 64, 64), :]
                f = turns - jnp.round(turns)
                f2 = f * f
                s = f * (SINE[0] + f2 * (SINE[1] + f2 * (SINE[2] + f2 * SINE[3])))
                p = s * s
                v = 2.0 - p
                co = 1.0 - p
                si = s * (v * lax.rsqrt(v))
                cosine[half, here, lanes] = co
                sine[half, here, lanes] = si
                re, im = charges * co, charges * si
                if not first:
                    re, im = creal[here, :] + re, cimag[here, :] + im
                if last:
                    re = jnp.sum(re, axis=1, keepdims=True)
                    im = jnp.sum(im, axis=1, keepdims=True)
                    w = weight[here, :]
                    wre, wim = w * re, w * im
                    e = wre * re + wim * im
                    for part in range(8):
                        total = total + e[8 * part : 8 * part + 8]
                    re, im = wre, wim
                creal[here, :] = re
                cimag[here, :] = im
            angle[1 - slot] = following
            return total

        return lax.fori_loop(0, blocks, step, jnp.zeros((8, LANES), jnp.float32))

    all_charges = []
    for chunk in range(chunks):
        for slot in range(8 * chunk, 8 * chunk + 8):
            if slot:
                sends[slot].wait_recv()
        parts, charges = unpack(chunk)
        all_charges.append(charges)
        total = phase_one(chunk, parts, charges, chunk == 0, chunk == chunks - 1)
    energy_row = jnp.sum(total, axis=0, keepdims=True) * (1.0 / (nsites * kvecs_all))
    scale = 4.0 * math.pi / math.sqrt(nsites * kvecs_all) / math.sqrt(nsites)

    posts = [None] * len(slots)
    for half in range(chunks // 2 - 1, -1, -1):

        def gather(block, total):
            here = pl.ds(pl.multiple_of(block * BLOCK, BLOCK), BLOCK)
            re, im = creal[here, :], cimag[here, :]
            parts = []
            for side in range(2):
                lanes = pl.ds(side * LANES, LANES)
                parts.append(sine[half, here, lanes] * re - cosine[half, here, lanes] * im)
            g = jnp.concatenate(parts, axis=1)
            high = g.astype(jnp.bfloat16)
            low = (g - high.astype(jnp.float32)).astype(jnp.bfloat16)
            m = xrows[:, here]
            return (
                total
                + jnp.dot(m, high, preferred_element_type=jnp.float32)
                + jnp.dot(m, low, preferred_element_type=jnp.float32)
            )

        force = lax.fori_loop(0, blocks, gather, jnp.zeros((16, 2 * LANES), jnp.float32), unroll=4)
        for side in (1, 0):
            chunk = 2 * half + side
            mine = force[0:3, side * LANES : (side + 1) * LANES] * (all_charges[chunk] * scale)
            outbox[chunk] = jnp.concatenate([mine, energy_row], axis=0)
        for side in (1, 0):
            chunk = 2 * half + side
            for slot in range(8 * chunk + 7, 8 * chunk - 1, -1):
                if slot == 0:
                    continue
                dz, dy = slots[slot]
                copy = pltpu.make_async_remote_copy(
                    src_ref=outbox.at[chunk],
                    dst_ref=inbox.at[slot],
                    send_sem=force_send.at[slot],
                    recv_sem=force_recv.at[slot],
                    device_id=at(nz - dz, ny - dy, 0, 0),
                    device_id_type=MESH,
                )
                copy.start()
                posts[slot] = copy

    row4 = lax.broadcasted_iota(jnp.int32, (4, LANES), 0)
    lane4 = lax.broadcasted_iota(jnp.int32, (4, LANES), 1)
    picked = jnp.zeros((4, LANES), jnp.float32)
    for s in range(8):
        own = None
        for chunk in range(chunks):
            slot = 8 * chunk + s
            if slot:
                posts[slot].wait_recv()
            value = inbox[slot] if slot else outbox[0]
            own = value if own is None else own + value
        picked = picked + jnp.where((row4 == 3) | (lane4 // GROUP == s), own, 0.0)
    shared[0] = picked
    lasts = []
    for mate, (dx, dc) in enumerate(mates):
        if mate:
            copy = pltpu.make_async_remote_copy(
                src_ref=shared.at[0],
                dst_ref=shared.at[mate],
                send_sem=last_send.at[mate],
                recv_sem=last_recv.at[mate],
                device_id=at(0, 0, dx, dc),
                device_id_type=MESH,
            )
            copy.start()
            lasts.append(copy)
    for copy in lasts:
        copy.wait_recv()
    whole = jnp.sum(shared[...], axis=0)
    per = forces.shape[1]
    mine = (x * nc + c) * per
    spot = lane4 % GROUP
    column = lax.broadcasted_iota(jnp.int32, (4, per), 1)
    out = jnp.zeros((4, per), jnp.float32)
    for index in range(per):
        value = jnp.sum(jnp.where(spot == mine + index, whole, 0.0), axis=1, keepdims=True)
        out = jnp.where(column == index, value, out)
    forces[...] = out[0:3]
    energy[...] = whole[3:4, 0:1]
    for copy in sends[1:] + posts[1:] + lasts:
        copy.wait_send()


def local(sizes, positions, site_class, class_charge, miller):
    nz, ny, nx, nc = sizes
    nslots, nmates = nz * ny, nx * nc
    kvecs = miller.shape[1] // nslots
    halves = nslots // 16
    vmem = pl.BlockSpec(memory_space=pltpu.VMEM)
    f32, bf16 = jnp.float32, jnp.bfloat16
    forces, energy = pl.pallas_call(
        functools.partial(kernel, sizes, miller.shape[1] * nmates),
        out_shape=(
            jax.ShapeDtypeStruct((3, positions.shape[1] // nmates), f32),
            jax.ShapeDtypeStruct((1, 1), f32),
        ),
        in_specs=[vmem, vmem, pl.BlockSpec(memory_space=pltpu.SMEM), pl.BlockSpec(memory_space=pl.ANY)],
        out_specs=(vmem, vmem),
        scratch_shapes=[
            pltpu.VMEM((3, kvecs), jnp.int32),
            pltpu.VMEM((16, kvecs), bf16),
            pltpu.VMEM((kvecs, 16), bf16),
            pltpu.VMEM((kvecs, LANES), f32),
            pltpu.VMEM((nslots, 1, LANES), f32),
            pltpu.VMEM((2, BLOCK, LANES), f32),
            pltpu.VMEM((halves, kvecs, 2 * LANES), f32),
            pltpu.VMEM((halves, kvecs, 2 * LANES), f32),
            pltpu.VMEM((kvecs, LANES), f32),
            pltpu.VMEM((kvecs, LANES), f32),
            pltpu.VMEM((nslots // 8, 4, LANES), f32),
            pltpu.VMEM((nslots, 4, LANES), f32),
            pltpu.VMEM((nmates, 4, LANES), f32),
            pltpu.SemaphoreType.DMA,
            pltpu.SemaphoreType.DMA((nslots,)),
            pltpu.SemaphoreType.DMA((nslots,)),
            pltpu.SemaphoreType.DMA((nslots,)),
            pltpu.SemaphoreType.DMA((nslots,)),
            pltpu.SemaphoreType.DMA((nmates,)),
            pltpu.SemaphoreType.DMA((nmates,)),
        ],
        compiler_params=pltpu.CompilerParams(
            collective_id=0, has_side_effects=True, vmem_limit_bytes=56 * 1024 * 1024
        ),
        name="ewald",
    )(positions, site_class.reshape(1, -1), class_charge, miller)
    return forces, energy.reshape(())


def solution(mesh):
    sizes = (8, 4, 4, 2)
    torus = Mesh(mesh.devices.reshape(sizes), AXES)
    placed = (P(None, SITE), P(SITE), P(), P(None, KA))
    return jax.shard_map(
        functools.partial(local, sizes),
        mesh=torus,
        in_specs=placed,
        out_specs=(P(None, SITE_KA), P()),
        check_vma=False,
    )
```

```python
import functools
import math

import jax
import jax.numpy as jnp
from jax import lax
from jax.experimental import pallas as pl
from jax.experimental.pallas import tpu as pltpu
from jax.sharding import Mesh
from jax.sharding import PartitionSpec as P

MMAX = 80
NCLS = 4
SITE = ("site_0", "site_1")
KA = ("ka_0", "ka_1")
SITE_KA = ("site_0", "site_1", "ka_0", "ka_1")
AXES = SITE_KA
MESH = pl.DeviceIdType.MESH
BLOCK = 256
STRIDE = 1024
LANES = 128
GROUP = 16
SINE = (4.442840086703501, -7.306690622039078, 3.589268246765133, -0.7724978545428361)


def offsets(far, near):
    steps = [(a, b) for a in range(far) for b in range(near)]
    return sorted(steps, key=lambda s: (min(s[0], far - s[0]) + min(s[1], near - s[1]), s))


def rounded(value):
    return value.astype(jnp.bfloat16).astype(jnp.float32)


def three_parts(value):
    high = rounded(value)
    middle = rounded(value - high)
    return high, middle, value - high - middle


def kernel(
    sizes,
    kvecs_all,
    positions,
    site_class,
    class_charge,
    miller,
    forces,
    energy,
    mints,
    xrows,
    columns,
    weight,
    table,
    angle,
    cosine,
    sine,
    creal,
    cimag,
    outbox,
    inbox,
    shared,
    mine_sem,
    site_send,
    site_recv,
    force_send,
    force_recv,
    last_send,
    last_recv,
):
    nz, ny, nx, nc = sizes
    kvecs = mints.shape[1]
    blocks = kvecs // BLOCK
    slots = offsets(nz, ny)
    mates = offsets(nx, nc)
    chunks = len(slots) // 8
    nsites = len(slots) * GROUP
    z, y, x, c = (lax.axis_index(axis) for axis in AXES)

    def at(dz, dy, dx, dc):
        return (lax.rem(z + dz, nz), lax.rem(y + dy, ny), lax.rem(x + dx, nx), lax.rem(c + dc, nc))

    start = pl.multiple_of((z * ny + y) * kvecs, LANES)
    fetch = pltpu.make_async_copy(miller.at[:, pl.ds(start, kvecs)], mints, mine_sem)
    fetch.start()
    barrier = pltpu.get_barrier_semaphore()
    for dz, dy in slots[:0:-1]:
        pl.semaphore_signal(barrier, inc=1, device_id=at(dz, dy, 0, 0), device_id_type=MESH)
    for dx, dc in mates[1:]:
        pl.semaphore_signal(barrier, inc=1, device_id=at(0, 0, dx, dc), device_id_type=MESH)

    classes = site_class[...]
    charge = jnp.zeros(classes.shape, jnp.float32)
    for index in range(NCLS):
        charge = jnp.where(classes == index, class_charge[index], charge)
    place = positions[...]
    place = place - jnp.round(place)
    table[0] = jnp.concatenate(
        [place[0:1], place[1:2], place[2:3], charge, jnp.zeros((1, LANES - 4 * GROUP), jnp.float32)], axis=1
    )

    pl.semaphore_wait(barrier, len(slots) + len(mates) - 2)
    sends = [None] * len(slots)
    for slot in range(len(slots) - 1, 0, -1):
        dz, dy = slots[slot]
        sends[slot] = pltpu.make_async_remote_copy(
            src_ref=table.at[0],
            dst_ref=table.at[slot],
            send_sem=site_send.at[slot],
            recv_sem=site_recv.at[slot],
            device_id=at(dz, dy, 0, 0),
            device_id_type=MESH,
        )
        sends[slot].start()

    fetch.wait()
    limit = float(MMAX * MMAX)

    def prepare(block, carry):
        here = pl.ds(pl.multiple_of(block * BLOCK, BLOCK), BLOCK)
        m = mints[:, here].astype(jnp.float32)
        square = m[0:1] * m[0:1] + m[1:2] * m[1:2] + m[2:3] * m[2:3]
        w = limit * jnp.exp(-square / limit) / square
        rows = jnp.concatenate([m, m, m, *three_parts(w), jnp.zeros((4, BLOCK), jnp.float32)], axis=0)
        xrows[:, here] = rows.astype(jnp.bfloat16)
        columns[here, :] = rows.T.astype(jnp.bfloat16)
        return carry

    lax.fori_loop(0, blocks, prepare, 0)
    row = lax.broadcasted_iota(jnp.int32, (16, LANES), 0)
    picks = jnp.where((row >= 9) & (row < 12), 1.0, 0.0).astype(jnp.bfloat16)

    def spread(block, carry):
        here = pl.ds(pl.multiple_of(block * BLOCK, BLOCK), BLOCK)
        weight[here, :] = jnp.dot(columns[here, :], picks, preferred_element_type=jnp.float32)
        return carry

    lax.fori_loop(0, blocks, spread, 0)

    lane = lax.broadcasted_iota(jnp.int32, (8, LANES), 1)
    sublane = lax.broadcasted_iota(jnp.int32, (8, LANES), 0)
    group = lane // GROUP

    def unpack(chunk):
        got = table[pl.ds(8 * chunk, 8), 0, :]
        rolled = [got if r == 0 else pltpu.roll(got, GROUP * r, axis=1) for r in range(8)]
        out = []
        for d in range(4):
            value = jnp.zeros((8, LANES), jnp.float32)
            for s in range(8):
                value = jnp.where((sublane == s) & (group == s), rolled[(s - d) % 8], value)
            out.append(jnp.sum(value, axis=0, keepdims=True))
        coords = jnp.concatenate(out[:3], axis=0)
        parts = jnp.concatenate([*three_parts(coords), jnp.zeros((7, LANES), jnp.float32)], axis=0)
        return parts.astype(jnp.bfloat16), out[3]

    strides = kvecs // STRIDE

    def angles(block, parts):
        here = pl.ds(pl.multiple_of(block * STRIDE, STRIDE), STRIDE)
        return jnp.dot(columns[here, :], parts, preferred_element_type=jnp.float32)

    def phase_one(chunk, parts, charges, first, last):
        half, lanes = chunk // 2, pl.ds((chunk % 2) * LANES, LANES)
        angle[0] = angles(0, parts)

        def step(block, total):
            following = angles(lax.rem(block + 1, strides), parts)
            slot = lax.rem(block, 2)
            base = block * STRIDE
            for sub in range(STRIDE // 64):
                here = pl.ds(pl.multiple_of(base + sub * 64, 64), 64)
                turns = angle[slot, pl.ds(sub * 64, 64), :]
                f = turns - jnp.round(turns)
                f2 = f * f
                s = f * (SINE[0] + f2 * (SINE[1] + f2 * (SINE[2] + f2 * SINE[3])))
                p = s * s
                v = 2.0 - p
                co = 1.0 - p
                si = s * (v * lax.rsqrt(v))
                cosine[half, here, lanes] = co
                sine[half, here, lanes] = si
                re, im = charges * co, charges * si
                if not first:
                    re, im = creal[here, :] + re, cimag[here, :] + im
                if last:
                    re = jnp.sum(re, axis=1, keepdims=True)
                    im = jnp.sum(im, axis=1, keepdims=True)
                    w = weight[here, :]
                    wre, wim = w * re, w * im
                    e = wre * re + wim * im
                    for part in range(8):
                        total = total + e[8 * part : 8 * part + 8]
                    re, im = wre, wim
                creal[here, :] = re
                cimag[here, :] = im
            angle[1 - slot] = following
            return total

        return lax.fori_loop(0, strides, step, jnp.zeros((8, LANES), jnp.float32))

    all_charges = []
    for chunk in range(chunks):
        for slot in range(8 * chunk, 8 * chunk + 8):
            if slot:
                sends[slot].wait_recv()
        parts, charges = unpack(chunk)
        all_charges.append(charges)
        total = phase_one(chunk, parts, charges, chunk == 0, chunk == chunks - 1)
    energy_row = jnp.sum(total, axis=0, keepdims=True) * (1.0 / (nsites * kvecs_all))
    scale = 4.0 * math.pi / math.sqrt(nsites * kvecs_all) / math.sqrt(nsites)

    posts = [None] * len(slots)
    for half in range(chunks // 2 - 1, -1, -1):

        def gather(block, total):
            here = pl.ds(pl.multiple_of(block * BLOCK, BLOCK), BLOCK)
            re, im = creal[here, :], cimag[here, :]
            parts = []
            for side in range(2):
                lanes = pl.ds(side * LANES, LANES)
                parts.append(sine[half, here, lanes] * re - cosine[half, here, lanes] * im)
            g = jnp.concatenate(parts, axis=1)
            high = g.astype(jnp.bfloat16)
            low = (g - high.astype(jnp.float32)).astype(jnp.bfloat16)
            m = xrows[:, here]
            return (
                total
                + jnp.dot(m, high, preferred_element_type=jnp.float32)
                + jnp.dot(m, low, preferred_element_type=jnp.float32)
            )

        force = lax.fori_loop(0, blocks, gather, jnp.zeros((16, 2 * LANES), jnp.float32), unroll=True)
        for side in (1, 0):
            chunk = 2 * half + side
            mine = force[0:3, side * LANES : (side + 1) * LANES] * (all_charges[chunk] * scale)
            outbox[chunk] = jnp.concatenate([mine, energy_row], axis=0)
        for side in (1, 0):
            chunk = 2 * half + side
            for slot in range(8 * chunk + 7, 8 * chunk - 1, -1):
                if slot == 0:
                    continue
                dz, dy = slots[slot]
                copy = pltpu.make_async_remote_copy(
                    src_ref=outbox.at[chunk],
                    dst_ref=inbox.at[slot],
                    send_sem=force_send.at[slot],
                    recv_sem=force_recv.at[slot],
                    device_id=at(nz - dz, ny - dy, 0, 0),
                    device_id_type=MESH,
                )
                copy.start()
                posts[slot] = copy

    for copy in sends[1:]:
        copy.wait_send()
    row4 = lax.broadcasted_iota(jnp.int32, (4, LANES), 0)
    lane4 = lax.broadcasted_iota(jnp.int32, (4, LANES), 1)
    picked = jnp.zeros((4, LANES), jnp.float32)
    for s in range(8):
        own = None
        for chunk in range(chunks):
            slot = 8 * chunk + s
            if slot:
                posts[slot].wait_recv()
            value = inbox[slot] if slot else outbox[0]
            own = value if own is None else own + value
        picked = picked + jnp.where((row4 == 3) | (lane4 // GROUP == s), own, 0.0)
    shared[0] = picked
    lasts = []
    for mate, (dx, dc) in enumerate(mates):
        if mate:
            copy = pltpu.make_async_remote_copy(
                src_ref=shared.at[0],
                dst_ref=shared.at[mate],
                send_sem=last_send.at[mate],
                recv_sem=last_recv.at[mate],
                device_id=at(0, 0, dx, dc),
                device_id_type=MESH,
            )
            copy.start()
            lasts.append(copy)
    for copy in posts[1:]:
        copy.wait_send()
    for copy in lasts:
        copy.wait_recv()
    whole = jnp.sum(shared[...], axis=0)
    per = forces.shape[0]
    mine = (x * nc + c) * per
    spot = lane4 % GROUP
    out = []
    for index in range(per):
        value = jnp.sum(jnp.where(spot == mine + index, whole, 0.0), axis=1, keepdims=True)
        out.append(jnp.sum(jnp.where(lane4 == row4, value, 0.0), axis=0, keepdims=True))
    forces[...] = jnp.concatenate(out, axis=0)[:, 0:3]
    energy[...] = whole[3:4, 0:1]
    for copy in lasts:
        copy.wait_send()


def local(sizes, positions, site_class, class_charge, miller):
    nz, ny, nx, nc = sizes
    nslots, nmates = nz * ny, nx * nc
    kvecs = miller.shape[1] // nslots
    halves = nslots // 16
    vmem = pl.BlockSpec(memory_space=pltpu.VMEM)
    f32, bf16 = jnp.float32, jnp.bfloat16
    forces, energy = pl.pallas_call(
        functools.partial(kernel, sizes, miller.shape[1] * nmates),
        out_shape=(
            jax.ShapeDtypeStruct((positions.shape[1] // nmates, 3), f32),
            jax.ShapeDtypeStruct((1, 1), f32),
        ),
        in_specs=[vmem, vmem, pl.BlockSpec(memory_space=pltpu.SMEM), pl.BlockSpec(memory_space=pl.ANY)],
        out_specs=(vmem, vmem),
        scratch_shapes=[
            pltpu.VMEM((3, kvecs), jnp.int32),
            pltpu.VMEM((16, kvecs), bf16),
            pltpu.VMEM((kvecs, 16), bf16),
            pltpu.VMEM((kvecs, LANES), f32),
            pltpu.VMEM((nslots, 1, LANES), f32),
            pltpu.VMEM((2, STRIDE, LANES), f32),
            pltpu.VMEM((halves, kvecs, 2 * LANES), f32),
            pltpu.VMEM((halves, kvecs, 2 * LANES), f32),
            pltpu.VMEM((kvecs, LANES), f32),
            pltpu.VMEM((kvecs, LANES), f32),
            pltpu.VMEM((nslots // 8, 4, LANES), f32),
            pltpu.VMEM((nslots, 4, LANES), f32),
            pltpu.VMEM((nmates, 4, LANES), f32),
            pltpu.SemaphoreType.DMA,
            pltpu.SemaphoreType.DMA((nslots,)),
            pltpu.SemaphoreType.DMA((nslots,)),
            pltpu.SemaphoreType.DMA((nslots,)),
            pltpu.SemaphoreType.DMA((nslots,)),
            pltpu.SemaphoreType.DMA((nmates,)),
            pltpu.SemaphoreType.DMA((nmates,)),
        ],
        compiler_params=pltpu.CompilerParams(
            collective_id=0, has_side_effects=True, vmem_limit_bytes=56 * 1024 * 1024
        ),
        name="ewald",
    )(positions, site_class.reshape(1, -1), class_charge, miller)
    return forces.T, energy.reshape(())


def solution(mesh):
    sizes = (8, 4, 4, 2)
    torus = Mesh(mesh.devices.reshape(sizes), AXES)
    placed = (P(None, SITE), P(SITE), P(), P(None, KA))
    return jax.shard_map(
        functools.partial(local, sizes),
        mesh=torus,
        in_specs=placed,
        out_specs=(P(None, SITE_KA), P()),
        check_vma=False,
    )
```

```python
import functools
import math

import jax
import jax.numpy as jnp
from jax import lax
from jax.experimental import pallas as pl
from jax.experimental.pallas import tpu as pltpu
from jax.sharding import Mesh
from jax.sharding import PartitionSpec as P

MMAX = 80
NCLS = 4
SITE = ("site_0", "site_1")
KA = ("ka_0", "ka_1")
SITE_KA = ("site_0", "site_1", "ka_0", "ka_1")
AXES = SITE_KA
MESH = pl.DeviceIdType.MESH
BLOCK = 256
STRIDE = 512
LANES = 128
GROUP = 16
SINE = (4.442840086703501, -7.306690622039078, 3.589268246765133, -0.7724978545428361)


def offsets(far, near):
    steps = [(a, b) for a in range(far) for b in range(near)]
    return sorted(steps, key=lambda s: (min(s[0], far - s[0]) + min(s[1], near - s[1]), s))


def rounded(value):
    return value.astype(jnp.bfloat16).astype(jnp.float32)


def three_parts(value):
    high = rounded(value)
    middle = rounded(value - high)
    return high, middle, value - high - middle


def kernel(
    sizes,
    positions,
    site_class,
    class_charge,
    miller,
    forces,
    energy,
    held_place,
    held_class,
    held_charge,
    mints,
    xrows,
    columns,
    weight,
    table,
    angle_a,
    angle_b,
    cosine,
    sine,
    creal,
    cimag,
    outbox,
    inbox,
    shared,
    mine_sem,
    site_send,
    site_recv,
    force_send,
    force_recv,
    last_send,
    last_recv,
):
    nz, ny, nx, nc = sizes
    kvecs = mints.shape[1]
    blocks = kvecs // BLOCK
    slots = offsets(nz, ny)
    mates = offsets(nx, nc)
    chunks = len(slots) // 8
    z, y, x, c = (lax.axis_index(axis) for axis in AXES)

    def at(dz, dy, dx, dc):
        return (lax.rem(z + dz, nz), lax.rem(y + dy, ny), lax.rem(x + dx, nx), lax.rem(c + dc, nc))

    barrier = pltpu.get_barrier_semaphore()
    for dz, dy in slots[:0:-1]:
        pl.semaphore_signal(barrier, inc=1, device_id=at(dz, dy, 0, 0), device_id_type=MESH)
    for dx, dc in mates[1:]:
        pl.semaphore_signal(barrier, inc=1, device_id=at(0, 0, dx, dc), device_id_type=MESH)
    start = pl.multiple_of((z * ny + y) * kvecs, LANES)
    fetches = [
        pltpu.make_async_copy(source, target, mine_sem.at[index])
        for index, (source, target) in enumerate(
            (
                (positions, held_place),
                (site_class, held_class),
                (class_charge, held_charge),
                (miller.at[:, pl.ds(start, kvecs)], mints),
            )
        )
    ]
    for fetch in fetches:
        fetch.start()
    for fetch in fetches[:3]:
        fetch.wait()

    classes = held_class[...]
    charge = jnp.zeros(classes.shape, jnp.float32)
    for index in range(NCLS):
        charge = jnp.where(classes == index, held_charge[index], charge)
    place = held_place[...]
    place = place - jnp.round(place)
    table[0] = jnp.concatenate(
        [place[0:1], place[1:2], place[2:3], charge, jnp.zeros((1, LANES - 4 * GROUP), jnp.float32)], axis=1
    )

    pl.semaphore_wait(barrier, len(slots) + len(mates) - 2)
    for slot in range(len(slots) - 1, 0, -1):
        dz, dy = slots[slot]
        pltpu.make_async_remote_copy(
            src_ref=table.at[0],
            dst_ref=table.at[slot],
            send_sem=site_send,
            recv_sem=site_recv.at[slot // 8],
            device_id=at(dz, dy, 0, 0),
            device_id_type=MESH,
        ).start()

    fetches[3].wait()
    limit = float(MMAX * MMAX)
    row = lax.broadcasted_iota(jnp.int32, (16, LANES), 0)
    picks = jnp.where((row >= 9) & (row < 12), 1.0, 0.0).astype(jnp.bfloat16)

    def prepare(block, carry):
        here = pl.ds(pl.multiple_of(block * BLOCK, BLOCK), BLOCK)
        m = mints[:, here].astype(jnp.float32)
        square = m[0:1] * m[0:1] + m[1:2] * m[1:2] + m[2:3] * m[2:3]
        w = limit * jnp.exp(-square / limit) / square
        rows = jnp.concatenate([m, m, m, *three_parts(w), jnp.zeros((4, BLOCK), jnp.float32)], axis=0)
        xrows[:, here] = rows.astype(jnp.bfloat16)
        turned = rows.T.astype(jnp.bfloat16)
        columns[here, :] = turned
        weight[here, :] = jnp.dot(turned, picks, preferred_element_type=jnp.float32)
        return carry

    lax.fori_loop(0, blocks, prepare, 0, unroll=True)

    lane = lax.broadcasted_iota(jnp.int32, (8, LANES), 1)
    sublane = lax.broadcasted_iota(jnp.int32, (8, LANES), 0)
    group = lane // GROUP

    def unpack(chunk):
        got = table[pl.ds(8 * chunk, 8), 0, :]
        rolled = [got if r == 0 else pltpu.roll(got, GROUP * r, axis=1) for r in range(8)]
        out = []
        for d in range(4):
            value = jnp.zeros((8, LANES), jnp.float32)
            for s in range(8):
                value = jnp.where((sublane == s) & (group == s), rolled[(s - d) % 8], value)
            out.append(jnp.sum(value, axis=0, keepdims=True))
        coords = jnp.concatenate(out[:3], axis=0)
        parts = jnp.concatenate([*three_parts(coords), jnp.zeros((7, LANES), jnp.float32)], axis=0)
        return parts.astype(jnp.bfloat16), out[3]

    strides = kvecs // STRIDE

    def angles(block, parts):
        here = pl.ds(pl.multiple_of(block * STRIDE, STRIDE), STRIDE)
        return jnp.dot(columns[here, :], parts, preferred_element_type=jnp.float32)

    def phase_one(chunk, parts, charges, first, last):
        half, lanes = chunk // 2, pl.ds((chunk % 2) * LANES, LANES)
        angle_a[...] = angles(0, parts)

        def process(angle, base, total):
            for sub in range(STRIDE // 64):
                here = pl.ds(pl.multiple_of(base + sub * 64, 64), 64)
                turns = angle[pl.ds(sub * 64, 64), :]
                f = turns - jnp.round(turns)
                f2 = f * f
                s = f * (SINE[0] + f2 * (SINE[1] + f2 * (SINE[2] + f2 * SINE[3])))
                p = s * s
                v = 2.0 - p
                co = 1.0 - p
                si = s * (v * lax.rsqrt(v))
                cosine[half, here, lanes] = co
                sine[half, here, lanes] = si
                re, im = charges * co, charges * si
                if not first:
                    re, im = creal[here, :] + re, cimag[here, :] + im
                if last:
                    re = jnp.sum(re, axis=1, keepdims=True)
                    im = jnp.sum(im, axis=1, keepdims=True)
                    w = weight[here, :]
                    wre, wim = w * re, w * im
                    e = wre * re + wim * im
                    for part in range(8):
                        total = total + e[8 * part : 8 * part + 8]
                    re, im = wre, wim
                creal[here, :] = re
                cimag[here, :] = im
            return total

        def step(pair, total):
            angle_b[...] = angles(2 * pair + 1, parts)
            total = process(angle_a, 2 * pair * STRIDE, total)
            angle_a[...] = angles(lax.rem(2 * pair + 2, strides), parts)
            return process(angle_b, (2 * pair + 1) * STRIDE, total)

        return lax.fori_loop(0, strides // 2, step, jnp.zeros((8, LANES), jnp.float32))

    def arrived(ref, chunk, sems):
        span = ref.at[pl.ds(max(8 * chunk, 1), 8 if chunk else 7)]
        pltpu.make_async_copy(span, span, sems.at[chunk]).wait()

    def departed(ref, sem):
        span = ref.at[pl.ds(1, ref.shape[0] - 1)]
        pltpu.make_async_copy(span, span, sem).wait()

    all_charges = []
    for chunk in range(chunks):
        arrived(table, chunk, site_recv)
        parts, charges = unpack(chunk)
        all_charges.append(charges)
        total = phase_one(chunk, parts, charges, chunk == 0, chunk == chunks - 1)
    energy_row = jnp.sum(total, axis=0, keepdims=True)

    for half in range(chunks // 2 - 1, -1, -1):

        def gather(block, total):
            here = pl.ds(pl.multiple_of(block * BLOCK, BLOCK), BLOCK)
            re, im = creal[here, :], cimag[here, :]
            parts = []
            for side in range(2):
                lanes = pl.ds(side * LANES, LANES)
                parts.append(sine[half, here, lanes] * re - cosine[half, here, lanes] * im)
            g = jnp.concatenate(parts, axis=1)
            high = g.astype(jnp.bfloat16)
            low = (g - high.astype(jnp.float32)).astype(jnp.bfloat16)
            m = xrows[:, here]
            return (
                total
                + jnp.dot(m, high, preferred_element_type=jnp.float32)
                + jnp.dot(m, low, preferred_element_type=jnp.float32)
            )

        force = lax.fori_loop(0, blocks, gather, jnp.zeros((16, 2 * LANES), jnp.float32), unroll=True)
        for side in (1, 0):
            chunk = 2 * half + side
            mine = force[0:3, side * LANES : (side + 1) * LANES] * all_charges[chunk]
            outbox[chunk] = jnp.concatenate([mine, energy_row], axis=0)
        for side in (1, 0):
            chunk = 2 * half + side
            for slot in range(8 * chunk + 7, 8 * chunk - 1, -1):
                if slot == 0:
                    continue
                dz, dy = slots[slot]
                pltpu.make_async_remote_copy(
                    src_ref=outbox.at[chunk],
                    dst_ref=inbox.at[slot],
                    send_sem=force_send,
                    recv_sem=force_recv.at[chunk],
                    device_id=at(nz - dz, ny - dy, 0, 0),
                    device_id_type=MESH,
                ).start()

    departed(table, site_send)
    row4 = lax.broadcasted_iota(jnp.int32, (4, LANES), 0)
    lane4 = lax.broadcasted_iota(jnp.int32, (4, LANES), 1)
    boxes = [None] * 8
    for chunk in range(chunks):
        arrived(inbox, chunk, force_recv)
        for s in range(8):
            value = inbox[8 * chunk + s] if chunk or s else outbox[0]
            boxes[s] = value if boxes[s] is None else boxes[s] + value
    picked = jnp.zeros((4, LANES), jnp.float32)
    for s in range(8):
        picked = picked + jnp.where((row4 == 3) | (lane4 // GROUP == s), boxes[s], 0.0)
    shared[0] = picked
    for mate in range(len(mates) - 1, 0, -1):
        dx, dc = mates[mate]
        pltpu.make_async_remote_copy(
            src_ref=shared.at[0],
            dst_ref=shared.at[mate],
            send_sem=last_send,
            recv_sem=last_recv,
            device_id=at(0, 0, dx, dc),
            device_id_type=MESH,
        ).start()
    departed(inbox, force_send)
    departed(shared, last_recv)
    whole = jnp.sum(shared[...], axis=0)
    per = forces.shape[0]
    mine = (x * nc + c) * per
    spot = lane4 % GROUP
    out = []
    for index in range(per):
        value = jnp.sum(jnp.where(spot == mine + index, whole, 0.0), axis=1, keepdims=True)
        out.append(jnp.sum(jnp.where(lane4 == row4, value, 0.0), axis=0, keepdims=True))
    forces[...] = jnp.concatenate(out, axis=0)[:, 0:3]
    energy[...] = whole[3:4, 0:1]
    departed(shared, last_send)


def local(sizes, positions, site_class, class_charge, miller):
    nz, ny, nx, nc = sizes
    nslots, nmates = nz * ny, nx * nc
    kvecs = miller.shape[1] // nslots
    halves = nslots // 16
    vmem = pl.BlockSpec(memory_space=pltpu.VMEM)
    f32, bf16 = jnp.float32, jnp.bfloat16
    forces, energy = pl.pallas_call(
        functools.partial(kernel, sizes),
        out_shape=(
            jax.ShapeDtypeStruct((positions.shape[1] // nmates, 3), f32),
            jax.ShapeDtypeStruct((1, 1), f32),
        ),
        in_specs=[pl.BlockSpec(memory_space=pl.ANY)] * 4,
        out_specs=(vmem, vmem),
        scratch_shapes=[
            pltpu.VMEM(positions.shape, f32),
            pltpu.VMEM((1, site_class.shape[0]), jnp.int32),
            pltpu.SMEM(class_charge.shape, f32),
            pltpu.VMEM((3, kvecs), jnp.int32),
            pltpu.VMEM((16, kvecs), bf16),
            pltpu.VMEM((kvecs, 16), bf16),
            pltpu.VMEM((kvecs, LANES), f32),
            pltpu.VMEM((nslots, 1, LANES), f32),
            pltpu.VMEM((STRIDE, LANES), f32),
            pltpu.VMEM((STRIDE, LANES), f32),
            pltpu.VMEM((halves, kvecs, 2 * LANES), f32),
            pltpu.VMEM((halves, kvecs, 2 * LANES), f32),
            pltpu.VMEM((kvecs, LANES), f32),
            pltpu.VMEM((kvecs, LANES), f32),
            pltpu.VMEM((nslots // 8, 4, LANES), f32),
            pltpu.VMEM((nslots, 4, LANES), f32),
            pltpu.VMEM((nmates, 4, LANES), f32),
            pltpu.SemaphoreType.DMA((4,)),
            pltpu.SemaphoreType.DMA,
            pltpu.SemaphoreType.DMA((nslots // 8,)),
            pltpu.SemaphoreType.DMA,
            pltpu.SemaphoreType.DMA((nslots // 8,)),
            pltpu.SemaphoreType.DMA,
            pltpu.SemaphoreType.DMA,
        ],
        compiler_params=pltpu.CompilerParams(
            collective_id=0, has_side_effects=True, vmem_limit_bytes=56 * 1024 * 1024
        ),
        name="ewald",
    )(positions, site_class.reshape(1, -1), class_charge, miller)
    nsites, kvecs_all = positions.shape[1] * nslots, miller.shape[1] * nmates
    scale = 4.0 * math.pi / math.sqrt(nsites * kvecs_all) / math.sqrt(nsites)
    return forces.T * scale, energy.reshape(()) * (1.0 / (nsites * kvecs_all))


def solution(mesh):
    sizes = (8, 4, 4, 2)
    torus = Mesh(mesh.devices.reshape(sizes), AXES)
    placed = (P(None, SITE), P(SITE), P(), P(None, KA))
    return jax.shard_map(
        functools.partial(local, sizes),
        mesh=torus,
        in_specs=placed,
        out_specs=(P(None, SITE_KA), P()),
        check_vma=False,
    )
```

```python
import functools
import math

import jax
import jax.numpy as jnp
from jax import lax
from jax.experimental import pallas as pl
from jax.experimental.pallas import tpu as pltpu
from jax.sharding import Mesh
from jax.sharding import PartitionSpec as P

MMAX = 80
NCLS = 4
SITE = ("site_0", "site_1")
KA = ("ka_0", "ka_1")
SITE_KA = ("site_0", "site_1", "ka_0", "ka_1")
AXES = SITE_KA
MESH = pl.DeviceIdType.MESH
BLOCK = 256
STRIDE = 4096
ROWS = 128
GROUPS = 3
LANES = 128
GROUP = 16
SINE = (0.7724978545428361, 0.9809405073019027, -3.66537433, 5.8630113)
SHY = 1.0 - 5.0e-7
TINY = 1.0e-30


def offsets(far, near):
    steps = [(a, b) for a in range(far) for b in range(near)]
    return sorted(steps, key=lambda s: (min(s[0], far - s[0]) + min(s[1], near - s[1]), s))


def rounded(value):
    return value.astype(jnp.bfloat16).astype(jnp.float32)


def three_parts(value):
    high = rounded(value)
    middle = rounded(value - high)
    return high, middle, value - high - middle


def kernel(
    sizes,
    positions,
    site_class,
    class_charge,
    miller,
    forces,
    energy,
    held_place,
    held_class,
    held_charge,
    mints,
    xrows,
    columns,
    weight,
    table,
    cosine,
    sine,
    creal,
    cimag,
    outbox,
    inbox,
    shared,
    mine_sem,
    site_send,
    site_recv,
    force_send,
    force_recv,
    last_send,
    last_recv,
):
    nz, ny, nx, nc = sizes
    kvecs = mints.shape[1]
    blocks = kvecs // BLOCK
    slots = offsets(nz, ny)
    mates = offsets(nx, nc)
    chunks = len(slots) // 8
    z, y, x, c = (lax.axis_index(axis) for axis in AXES)

    def at(dz, dy, dx, dc):
        return (lax.rem(z + dz, nz), lax.rem(y + dy, ny), lax.rem(x + dx, nx), lax.rem(c + dc, nc))

    barrier = pltpu.get_barrier_semaphore()
    for dz, dy in slots[:0:-1]:
        pl.semaphore_signal(barrier, inc=1, device_id=at(dz, dy, 0, 0), device_id_type=MESH)
    for dx, dc in mates[1:]:
        pl.semaphore_signal(barrier, inc=1, device_id=at(0, 0, dx, dc), device_id_type=MESH)
    start = pl.multiple_of((z * ny + y) * kvecs, LANES)
    fetches = [
        pltpu.make_async_copy(source, target, mine_sem.at[index])
        for index, (source, target) in enumerate(
            (
                (positions, held_place),
                (site_class, held_class),
                (class_charge, held_charge),
                (miller.at[:, pl.ds(start, kvecs)], mints),
            )
        )
    ]
    for fetch in fetches:
        fetch.start()
    for fetch in fetches[:3]:
        fetch.wait()

    classes = held_class[...]
    charge = jnp.zeros(classes.shape, jnp.float32)
    for index in range(NCLS):
        charge = jnp.where(classes == index, held_charge[index], charge)
    place = held_place[...]
    place = place - jnp.round(place)
    table[0] = jnp.concatenate(
        [place[0:1], place[1:2], place[2:3], charge, jnp.zeros((1, LANES - 4 * GROUP), jnp.float32)], axis=1
    )

    pl.semaphore_wait(barrier, len(slots) + len(mates) - 2)
    for slot in range(len(slots) - 1, 0, -1):
        dz, dy = slots[slot]
        pltpu.make_async_remote_copy(
            src_ref=table.at[0],
            dst_ref=table.at[slot],
            send_sem=site_send.at[slot * 2 // len(slots)],
            recv_sem=site_recv.at[slot // 8],
            device_id=at(dz, dy, 0, 0),
            device_id_type=MESH,
        ).start()

    fetches[3].wait()
    limit = float(MMAX * MMAX)
    row = lax.broadcasted_iota(jnp.int32, (16, LANES), 0)
    picks = jnp.where((row >= 9) & (row < 12), 1.0, 0.0).astype(jnp.bfloat16)

    def prepare(block, carry):
        here = pl.ds(pl.multiple_of(block * BLOCK, BLOCK), BLOCK)
        m = mints[:, here].astype(jnp.float32)
        square = m[0:1] * m[0:1] + m[1:2] * m[1:2] + m[2:3] * m[2:3]
        w = limit * jnp.exp(-square / limit) / square
        rows = jnp.concatenate([m, m, m, *three_parts(w), jnp.ones((4, BLOCK), jnp.float32)], axis=0)
        xrows[:, here] = rows.astype(jnp.bfloat16)
        turned = rows.T.astype(jnp.bfloat16)
        columns[here, :] = turned
        weight[here, :] = jnp.dot(turned, picks, preferred_element_type=jnp.float32)
        return carry

    lax.fori_loop(0, blocks, prepare, 0, unroll=True)

    lane = lax.broadcasted_iota(jnp.int32, (8, LANES), 1)
    sublane = lax.broadcasted_iota(jnp.int32, (8, LANES), 0)
    group = lane // GROUP

    def unpack(chunk):
        got = table[pl.ds(8 * chunk, 8), 0, :]
        rolled = [got if r == 0 else pltpu.roll(got, GROUP * r, axis=1) for r in range(8)]
        out = []
        for d in range(4):
            value = jnp.zeros((8, LANES), jnp.float32)
            for s in range(8):
                value = jnp.where((sublane == s) & (group == s), rolled[(s - d) % 8], value)
            out.append(jnp.sum(value, axis=0, keepdims=True))
        coords = jnp.concatenate(out[:3], axis=0)
        flip = jnp.where(out[3] < 0.0, 0.5, 0.0)
        none = jnp.zeros((3, LANES), jnp.float32)
        parts = jnp.concatenate([*three_parts(coords), none, flip, none], axis=0)
        size = jnp.maximum(jnp.abs(out[3]), TINY)
        return parts.astype(jnp.bfloat16), size, (SINE[0] * SHY) * jnp.sqrt(size)

    def phase_one(chunk, parts, size, amplitude, first, last):
        half, lanes = chunk // 2, pl.ds((chunk % 2) * LANES, LANES)
        twice = 2.0 * size

        def step(stride, total):
            base = stride * STRIDE
            for sub in range(STRIDE // ROWS):
                here = pl.ds(pl.multiple_of(base + sub * ROWS, ROWS), ROWS)
                turns = jnp.dot(columns[here, :], parts, preferred_element_type=jnp.float32)
                f = turns - jnp.round(turns)
                f2 = f * f
                s = (amplitude * f) * ((SINE[1] - f2) * ((f2 + SINE[2]) * f2 + SINE[3]))
                p = s * s
                v = twice - p
                re = size - p
                im = s * (v * lax.rsqrt(v))
                cosine[half, here, lanes] = re
                sine[half, here, lanes] = im
                if not first:
                    re, im = creal[here, :] + re, cimag[here, :] + im
                if last:
                    re = jnp.sum(re, axis=1, keepdims=True)
                    im = jnp.sum(im, axis=1, keepdims=True)
                    w = weight[here, :]
                    wre, wim = w * re, w * im
                    e = wre * re + wim * im
                    for part in range(ROWS // 8):
                        total = total + e[8 * part : 8 * part + 8]
                    re, im = wre, wim
                creal[here, :] = re
                cimag[here, :] = im
            return total

        return lax.fori_loop(0, kvecs // STRIDE, step, jnp.zeros((8, LANES), jnp.float32))

    def arrived(ref, chunk, sems):
        span = ref.at[pl.ds(max(8 * chunk, 1), 8 if chunk else 7)]
        pltpu.make_async_copy(span, span, sems.at[chunk]).wait()

    def departed(ref, sem, first, count):
        span = ref.at[pl.ds(first, count)]
        pltpu.make_async_copy(span, span, sem).wait()

    for chunk in range(chunks):
        arrived(table, chunk, site_recv)
        total = phase_one(chunk, *unpack(chunk), chunk == 0, chunk == chunks - 1)
    energy_row = jnp.sum(total, axis=0, keepdims=True)

    def phase_two(group):
        def gather(block, total):
            here = pl.ds(pl.multiple_of(block * BLOCK, BLOCK), BLOCK)
            re, im = creal[here, :], cimag[here, :]
            parts = []
            for chunk in group:
                half, lanes = chunk // 2, pl.ds((chunk % 2) * LANES, LANES)
                parts.append(sine[half, here, lanes] * re - cosine[half, here, lanes] * im)
            g = parts[0] if len(parts) == 1 else jnp.concatenate(parts, axis=1)
            high = g.astype(jnp.bfloat16)
            low = (g - high.astype(jnp.float32)).astype(jnp.bfloat16)
            m = xrows[:, here]
            return (
                total
                + jnp.dot(m, high, preferred_element_type=jnp.float32)
                + jnp.dot(m, low, preferred_element_type=jnp.float32)
            )

        force = lax.fori_loop(0, blocks, gather, jnp.zeros((16, len(group) * LANES), jnp.float32), unroll=True)
        for index, chunk in enumerate(group):
            outbox[chunk] = jnp.concatenate([force[0:3, index * LANES : (index + 1) * LANES], energy_row], axis=0)
        for chunk in group:
            for slot in range(8 * chunk + 7, 8 * chunk - 1, -1):
                if slot == 0:
                    continue
                dz, dy = slots[slot]
                pltpu.make_async_remote_copy(
                    src_ref=outbox.at[chunk],
                    dst_ref=inbox.at[slot],
                    send_sem=force_send,
                    recv_sem=force_recv.at[chunk],
                    device_id=at(nz - dz, ny - dy, 0, 0),
                    device_id_type=MESH,
                ).start()

    if GROUPS == 3:
        phase_two((3,))
        departed(table, site_send.at[1], len(slots) // 2, len(slots) // 2)
        phase_two((2,))
        departed(table, site_send.at[0], 1, len(slots) // 2 - 1)
        phase_two((1, 0))
    else:
        phase_two((3, 2))
        departed(table, site_send.at[1], len(slots) // 2, len(slots) // 2)
        departed(table, site_send.at[0], 1, len(slots) // 2 - 1)
        phase_two((1, 0))
    row4 = lax.broadcasted_iota(jnp.int32, (4, LANES), 0)
    lane4 = lax.broadcasted_iota(jnp.int32, (4, LANES), 1)
    boxes = [None] * 8
    for chunk in range(chunks):
        arrived(inbox, chunk, force_recv)
        for s in range(8):
            value = inbox[8 * chunk + s] if chunk or s else outbox[0]
            boxes[s] = value if boxes[s] is None else boxes[s] + value
    picked = jnp.zeros((4, LANES), jnp.float32)
    for s in range(8):
        picked = picked + jnp.where((row4 == 3) | (lane4 // GROUP == s), boxes[s], 0.0)
    shared[0] = picked
    for mate in range(len(mates) - 1, 0, -1):
        dx, dc = mates[mate]
        pltpu.make_async_remote_copy(
            src_ref=shared.at[0],
            dst_ref=shared.at[mate],
            send_sem=last_send,
            recv_sem=last_recv,
            device_id=at(0, 0, dx, dc),
            device_id_type=MESH,
        ).start()
    departed(inbox, force_send, 1, len(slots) - 1)
    departed(shared, last_recv, 1, len(mates) - 1)
    whole = jnp.sum(shared[...], axis=0)
    per = forces.shape[0]
    mine = (x * nc + c) * per
    spot = lane4 % GROUP
    out = []
    for index in range(per):
        value = jnp.sum(jnp.where(spot == mine + index, whole, 0.0), axis=1, keepdims=True)
        out.append(jnp.sum(jnp.where(lane4 == row4, value, 0.0), axis=0, keepdims=True))
    forces[...] = jnp.concatenate(out, axis=0)[:, 0:3]
    energy[...] = whole[3:4, 0:1]
    departed(shared, last_send, 1, len(mates) - 1)


def local(sizes, positions, site_class, class_charge, miller):
    nz, ny, nx, nc = sizes
    nslots, nmates = nz * ny, nx * nc
    kvecs = miller.shape[1] // nslots
    halves = nslots // 16
    vmem = pl.BlockSpec(memory_space=pltpu.VMEM)
    f32, bf16 = jnp.float32, jnp.bfloat16
    forces, energy = pl.pallas_call(
        functools.partial(kernel, sizes),
        out_shape=(
            pltpu.VMEM((positions.shape[1] // nmates, 3), f32),
            pltpu.VMEM((1, 1), f32),
        ),
        in_specs=[pl.BlockSpec(memory_space=pl.ANY)] * 4,
        out_specs=(vmem, vmem),
        scratch_shapes=[
            pltpu.VMEM(positions.shape, f32),
            pltpu.VMEM((1, site_class.shape[0]), jnp.int32),
            pltpu.SMEM(class_charge.shape, f32),
            pltpu.VMEM((3, kvecs), jnp.int32),
            pltpu.VMEM((16, kvecs), bf16),
            pltpu.VMEM((kvecs, 16), bf16),
            pltpu.VMEM((kvecs, LANES), f32),
            pltpu.VMEM((nslots, 1, LANES), f32),
            pltpu.VMEM((halves, kvecs, 2 * LANES), f32),
            pltpu.VMEM((halves, kvecs, 2 * LANES), f32),
            pltpu.VMEM((kvecs, LANES), f32),
            pltpu.VMEM((kvecs, LANES), f32),
            pltpu.VMEM((nslots // 8, 4, LANES), f32),
            pltpu.VMEM((nslots, 4, LANES), f32),
            pltpu.VMEM((nmates, 4, LANES), f32),
            pltpu.SemaphoreType.DMA((4,)),
            pltpu.SemaphoreType.DMA((2,)),
            pltpu.SemaphoreType.DMA((nslots // 8,)),
            pltpu.SemaphoreType.DMA,
            pltpu.SemaphoreType.DMA((nslots // 8,)),
            pltpu.SemaphoreType.DMA,
            pltpu.SemaphoreType.DMA,
        ],
        compiler_params=pltpu.CompilerParams(
            collective_id=0, has_side_effects=True, vmem_limit_bytes=56 * 1024 * 1024
        ),
        name="ewald",
    )(positions, site_class.reshape(1, -1), class_charge, miller)
    nsites, kvecs_all = positions.shape[1] * nslots, miller.shape[1] * nmates
    scale = 4.0 * math.pi / math.sqrt(nsites * kvecs_all) / math.sqrt(nsites)
    return forces.T * scale, energy.reshape(()) * (1.0 / (nsites * kvecs_all))


def solution(mesh):
    sizes = (8, 4, 4, 2)
    torus = Mesh(mesh.devices.reshape(sizes), AXES)
    placed = (P(None, SITE), P(SITE), P(), P(None, KA))
    return jax.shard_map(
        functools.partial(local, sizes),
        mesh=torus,
        in_specs=placed,
        out_specs=(P(None, SITE_KA), P()),
        check_vma=False,
    )
```
